32 devices in a mesh: prow: 8 (over y, x, core), pcol: 4 (over z).
Axes of the slice: x: 2, y: 2, z: 4, core: 2. Of those that a mesh axis runs over, the one named last changes fastest.
Arguments:
- ancestor_inverse: float32 [8, 8, 512, 512], P('prow', 'pcol'), may hold values from -0.09375 to 0.09375
- factor_panel: float32 [512, 8, 3, 512], P('pcol', 'prow'), may hold values from -0.75 to 0.75
- pivot_inverse: float32 [3, 512, 512], P(None, 'prow', 'pcol'), may hold values from -6 to 6
- structure: int32 [8, 3], replicated, may hold values from 0 to 1, as said below
Outputs:
- inverse_panel: float32 [512, 8, 3, 512], P('pcol', 'prow')
- diagonal_block: float32 [3, 512, 512], P(None, 'prow', 'pcol')
The draws below stay inside these ranges and needn't reach their ends.
Inputs may be any that keep to these rules, and one draw needn't show every extreme that they name: structure[J, K] is 1 where ancestor J lies in supernode K's structure and 0 elsewhere; the last ancestor, 7, lies in every supernode's structure.
All inputs are finite; a program needn't handle non-finite values.
Results may differ from the reference program's by a relative error of at most 0.00007.
Values sent between devices are 32-bit elements; how exact they have to be, the bound alone decides.
A program may use at most 64 MiB of HBM per device.

```python
import jax
import jax.numpy as jnp
from jax import lax

B = 512
SUPER = 3
M = 8


def draw_structure(key, part):
    drawn_levels = jax.random.randint(key, (M, SUPER), 0, M)
    ancestor_index = jnp.arange(M, dtype=jnp.int32)[:, None]
    return jnp.where(drawn_levels <= ancestor_index, 1, 0).astype(jnp.int32)


def level_of(rng, extent, shards, smallest, largest):
    level = 1.0
    for position, shards_of in shards:
        draws = jax.random.uniform(jax.random.fold_in(jax.random.fold_in(rng, 6), position), (shards_of,), jnp.float32, smallest / len(shards), largest / len(shards))
        level = level * jnp.repeat(jnp.exp(draws), extent[position] // shards_of).reshape((-1,) + (1,) * (len(extent) - 1 - position))
    return level


def gaussian(rng, shape, scale, limit, pieces=(), held_as=jnp.bfloat16):
    factor_of = level_of(rng, shape, pieces, -0.22, 0.18) if pieces else 1.0
    values = jax.random.normal(rng, shape, jnp.float32) * scale * factor_of
    return jnp.minimum(jnp.maximum(values, -limit), limit).astype(held_as)


def setup_inputs(seed: int = 0) -> dict:
    keys = jax.random.split(jax.random.key(seed), 5)
    return {
        "ancestor_inverse": gaussian(keys[0], (M, M, B, B), (M * B) ** -0.5, 0.09375, ((0, 8), (1, 4)), jnp.float32),
        "factor_panel": gaussian(keys[1], (B, M, SUPER, B), 0.125, 0.75, ((0, 4), (1, 8)), jnp.float32),
        "pivot_inverse": gaussian(keys[2], (SUPER, B, B), 1.0, 6.0, ((1, 8), (2, 4)), jnp.float32),
        "structure": draw_structure(jax.random.fold_in(keys[4], 71), 0),
    }


def reference(ancestor_inverse, factor_panel, pivot_inverse, structure):
    struct_float = structure.astype(jnp.float32)
    masked = factor_panel * struct_float[None, :, :, None]

    def one_row(inverse_row):
        return jnp.einsum("Jrt,tJKc->rKc", inverse_row, masked, precision=lax.Precision.HIGHEST, preferred_element_type=jnp.float32)

    product = lax.map(one_row, ancestor_inverse)
    product = jnp.transpose(product, (1, 0, 2, 3))
    inverse_panel = -struct_float[None, :, :, None] * product
    diagonal_block = pivot_inverse - jnp.einsum("riKa,riKb->Kab", masked, inverse_panel, precision=lax.Precision.HIGHEST, preferred_element_type=jnp.float32)
    return inverse_panel, diagonal_block
```

```python
import functools

import jax
import jax.numpy as jnp
from jax import lax
from jax.experimental import pallas as pl
from jax.experimental.pallas import tpu as pltpu
from jax.sharding import PartitionSpec as P

MESH = pl.DeviceIdType.MESH
PAIR = 2
PIECE = 128
AHEAD = 4
LAGS = {"across": -AHEAD, "along": -3, "spread": -2, "forward": -1, "multiply": 0}
CHAIN_LAG = 1
TAIL_LAG = 1


def split(value):
    high = value.astype(jnp.bfloat16)
    low = (value - high.astype(jnp.float32)).astype(jnp.bfloat16)
    return high, low


def dot(a, b):
    return lax.dot_general(a, b, (((1,), (0,)), ((), ())), preferred_element_type=jnp.float32)


def flip(value, number, size):
    bit, total = 1, value
    while bit < size:
        if (number // bit) % 2:
            here = lax.rem(lax.div(value, bit), 2)
            total = total + bit - 2 * bit * here
        bit *= 2
    return total


def flip_both(left, right, size):
    bit, total = 1, 0
    while bit < size:
        a, b = lax.rem(lax.div(left, bit), 2), lax.rem(lax.div(right, bit), 2)
        total = total + bit * (a + b - 2 * a * b)
        bit *= 2
    return total


def kernel(
    rows_n,
    cols_n,
    struct_hbm,
    factor_hbm,
    inverse_hbm,
    pivot_ref,
    panel_hbm,
    diag_ref,
    struct,
    raw,
    a_full,
    a_high,
    a_low,
    masked,
    turned,
    staged,
    columns,
    both,
    partial,
    chain_in,
    result_out,
    terms,
    pair_in,
    pair_sum,
    chip_in,
    cut,
    cut_in,
    load_sem,
    sends,
    hop_recv,
    near_recv,
    mate_recv,
    chain_recv,
    pair_recv,
    chip_recv,
    cut_recv,
):
    row = lax.axis_index("prow")
    col = lax.axis_index("pcol")
    chunks, rows, piece = masked.shape
    members, width = a_full.shape[0], a_full.shape[1]
    supers = struct.shape[0]
    per_super = width // piece
    chips = rows_n // PAIR
    part = width // rows_n
    lanes = width // cols_n
    cuts = piece // lanes
    core = lax.rem(row, PAIR)
    chip = lax.div(row, PAIR)
    mate = chip * PAIR + (1 - core)
    group = lax.div(row, members)
    member = lax.rem(row, members)
    both_ways = flip_both(group, col, cols_n)

    load_struct = pltpu.make_async_copy(struct_hbm, struct, load_sem.at[0])
    load_raw = pltpu.make_async_copy(factor_hbm, raw, load_sem.at[1])
    load_a = pltpu.make_async_copy(inverse_hbm.at[0], a_full, load_sem.at[2])
    store_panel = pltpu.make_async_copy(result_out, panel_hbm, load_sem.at[3])
    load_struct.start()
    load_raw.start()
    load_a.start()

    barrier = pltpu.get_barrier_semaphore()
    for step in range(1, rows_n):
        pl.semaphore_signal(
            barrier, inc=1, device_id={"prow": lax.rem(row + step, rows_n)}, device_id_type=MESH
        )
    for step in range(1, cols_n):
        pl.semaphore_signal(
            barrier, inc=1, device_id={"pcol": lax.rem(col + step, cols_n)}, device_id_type=MESH
        )

    def remote(src, dst, send, recv, where):
        return pltpu.make_async_remote_copy(
            src_ref=src, dst_ref=dst, send_sem=send, recv_sem=recv, device_id=where, device_id_type=MESH
        )

    sent = []

    def begin(copy, when=None):
        if when is None:
            copy.start()
        else:
            pl.when(when)(copy.start)
        sent.append((copy, when))

    def across(k):
        to_group = flip(flip_both(group, col, cols_n), k, cols_n)
        stays = flip(col, k, cols_n) == 0
        return (
            remote(
                masked.at[k],
                staged.at[k],
                sends.at[0],
                hop_recv.at[0, k],
                {"prow": to_group * members + member},
            ),
            stays,
        )

    def start_across(k):
        mask = struct[k // per_super, row].astype(jnp.float32)
        value = raw[pl.ds(k, rows, stride=chunks), :] * mask
        masked[k] = value
        copy, stays = across(k)

        @pl.when(stays)
        def _():
            staged[k] = value

        begin(copy, jnp.logical_not(stays))

    def slot_of(source, k):
        from_col = flip(flip_both(lax.div(source, members), col, cols_n), k, cols_n)
        return lax.rem(source, members) * cols_n + from_col

    def along(k):
        to_col = flip(both_ways, k, cols_n)
        copy = remote(
            staged.at[k],
            columns.at[k, member * cols_n + col],
            sends.at[1],
            hop_recv.at[1, k],
            {"pcol": to_col},
        )
        return copy, to_col == col

    def start_along(k):
        copy, stays = across(k)
        pl.when(jnp.logical_not(stays))(copy.wait_recv)
        copy, home = along(k)

        @pl.when(home)
        def _():
            columns[k, member * cols_n + col] = staged[k]

        begin(copy, jnp.logical_not(home))

    def near(k, source, target):
        here = columns.at[k, slot_of(source, k)]
        return remote(here, here, sends.at[2], near_recv.at[k], {"prow": target})

    def over(k, source):
        here = columns.at[k, slot_of(source, k)]
        return remote(here, here, sends.at[3], mate_recv.at[k], {"prow": mate})

    def arrived(buffer, index, count, semaphore):
        here = buffer.at[index, pl.ds(0, count)]
        return remote(here, here, sends.at[0], semaphore, {"prow": mate})

    def back(source, step):
        return lax.rem(source - PAIR * step + rows_n, rows_n)

    def start_spread(k):
        copy, home = along(k)
        pl.when(jnp.logical_not(home))(copy.wait_recv)
        for step in range(chips - 1, 0, -1):
            begin(near(k, row, lax.rem(row + PAIR * step, rows_n)))
        begin(over(k, row))

    def forward(k):
        arrived(columns, k, chips - 1, near_recv.at[k]).wait_recv()
        for step in range(1, chips):
            begin(over(k, back(row, step)))

    def multiply(k):
        arrived(columns, k, chips, mate_recv.at[k]).wait_recv()
        for index in range(members * cols_n):
            high, low = split(columns[k, index])
            both[index * rows : (index + 1) * rows, :piece] = high
            both[index * rows : (index + 1) * rows, piece:] = low
        first = dot(a_high[...], both[...])
        second = dot(a_low[...], both[:, :piece])
        partial[k] = first[:, :piece] + (first[:, piece:] + second)

    def chain_copy(k, step, side):
        place = col if side == 0 else cols_n - 1 - col
        block = cols_n - 1 - step + place
        block = block if side == 0 else cols_n - 1 - block
        at = pl.ds(pl.multiple_of(block * rows, rows), rows)
        copy = remote(
            partial.at[k, at],
            chain_in.at[k, side, step],
            sends.at[4],
            chain_recv.at[k, side, step],
            {"pcol": col + 1 - 2 * side},
        )
        return copy, at, place

    def came_from(k, step, side):
        return remote(
            chain_in.at[k, side, step],
            chain_in.at[k, side, step],
            sends.at[4],
            chain_recv.at[k, side, step],
            {"pcol": lax.rem(col + 1, cols_n)},
        )

    def chain(step, k):
        for side in (0, 1):
            copy, at, place = chain_copy(k, step, side)
            if step:

                @pl.when(jnp.logical_and(place > 0, place <= step))
                def _():
                    came_from(k, step - 1, side).wait_recv()
                    partial[k, at, :] = partial[k, at, :] + chain_in[k, side, step - 1]

            begin(copy, place <= step)

    def finish_panel(k):
        own = pl.ds(pl.multiple_of(col * rows, rows), rows)
        for side in (0, 1):
            place = col if side == 0 else cols_n - 1 - col

            @pl.when(place > 0)
            def _():
                came_from(k, cols_n - 2, side).wait_recv()
                partial[k, own, :] = partial[k, own, :] + chain_in[k, side, cols_n - 2]

        mask = struct[k // per_super, row].astype(jnp.float32)
        result = -mask * partial[k, own, :]
        result_out[pl.ds(k, rows, stride=chunks), :] = result
        if k == chunks - 1:
            store_panel.start()
        high, low = split(result)
        sides = jnp.concatenate([high, low], axis=1)
        first = dot(turned[k // per_super, 0], sides)
        second = dot(turned[k // per_super, 1], high)
        term = first[:, :piece] + (first[:, piece:] + second)
        for at in range(rows_n):
            terms[k, at % PAIR, at // PAIR] = term[at * part : (at + 1) * part]
        begin(pair_copy(k))

    def pair_copy(k):
        return remote(terms.at[k, 1 - core], pair_in.at[k], sends.at[5], pair_recv.at[k], {"prow": mate})

    def chip_copy(k, step):
        to_chip = lax.rem(chip + step, chips)
        return remote(
            pair_sum.at[k, to_chip],
            chip_in.at[k, step - 1],
            sends.at[6],
            chip_recv.at[k],
            {"prow": to_chip * PAIR + core},
        )

    def add_pair(k):
        pair_copy(k).wait_recv()
        pair_sum[k] = terms[k, core] + pair_in[k]
        for step in range(chips - 1, 0, -1):
            begin(chip_copy(k, step))

    def cut_copy(k, at, target):
        step = lax.rem(col - target + cols_n, cols_n)
        return remote(
            cut.at[k, at],
            cut_in.at[k, at, step],
            sends.at[7],
            cut_recv.at[k, at],
            {"pcol": target},
        )

    def add_chips(k):
        total = pair_sum[k, chip]
        arrived(chip_in, k, chips - 1, chip_recv.at[k]).wait_recv()
        for step in range(1, chips):
            total = total + chip_in[k, step - 1]
        for at in range(cuts):
            cut[k, at] = total[:, at * lanes : (at + 1) * lanes]
            target = k % per_super * cuts + at
            begin(cut_copy(k, at, target), col != target)

    def add_cuts(k):
        for at in range(cuts):

            @pl.when(col == k % per_super * cuts + at)
            def _():
                here = cut_in.at[k, at, pl.ds(1, cols_n - 1)]
                remote(here, here, sends.at[0], cut_recv.at[k, at], {"prow": mate}).wait_recv()
                total = cut[k, at]
                for step in range(1, cols_n):
                    total = total + cut_in[k, at, step]
                diag_ref[k // per_super] = pivot_ref[k // per_super] - total

    def prepare_a():
        load_a.wait()
        for index in range(members):
            high, low = split(a_full[index])
            a_high[:, index * width : (index + 1) * width] = high
            a_low[:, index * width : (index + 1) * width] = low

    def prepare_turned(s):
        for at in range(per_super):
            high, low = split(masked[s * per_super + at].T)
            turned[s, 0, at * piece : (at + 1) * piece] = high
            turned[s, 1, at * piece : (at + 1) * piece] = low

    steps = cols_n - 1
    stages = [("add_cuts", add_cuts, CHAIN_LAG * steps + 3 * TAIL_LAG)]
    stages.append(("add_chips", add_chips, CHAIN_LAG * steps + 2 * TAIL_LAG))
    stages.append(("add_pair", add_pair, CHAIN_LAG * steps + TAIL_LAG))
    stages.append(("finish", finish_panel, CHAIN_LAG * steps))
    for step in range(steps - 1, 0, -1):
        stages.append(("chain", functools.partial(chain, step), CHAIN_LAG * step))
    stages.append(("forward", forward, LAGS["forward"]))
    stages.append(("spread", start_spread, LAGS["spread"]))
    stages.append(("along", start_along, LAGS["along"]))
    stages.append(("across", start_across, LAGS["across"]))
    stages.append(("multiply", multiply, 0))
    stages.append(("chain", functools.partial(chain, 0), 0))
    last = max(lag for _, _, lag in stages)

    load_struct.wait()
    load_raw.wait()
    pl.semaphore_wait(barrier, rows_n + cols_n - 2)

    for wave in range(-AHEAD, chunks + last):
        for _, stage, lag in stages:
            if 0 <= wave - lag < chunks:
                stage(wave - lag)
        if wave == -2:
            prepare_a()
        for s in range(supers):
            if wave + AHEAD == (s + 1) * per_super - 1:
                prepare_turned(s)

    store_panel.wait()
    for copy, when in sent:
        if when is None:
            copy.wait_send()
        else:
            pl.when(when)(copy.wait_send)


def body(ancestor_inverse, factor_panel, pivot_inverse, structure):
    rows_n, cols_n = lax.axis_size("prow"), lax.axis_size("pcol")
    members, width = ancestor_inverse.shape[1], ancestor_inverse.shape[3]
    rows, _, supers, _ = factor_panel.shape
    chips, part, lanes = rows_n // PAIR, width // rows_n, width // cols_n
    piece = max(PIECE, lanes)
    chunks, cuts = supers * width // piece, piece // lanes
    factor = factor_panel.reshape(rows * chunks, piece)
    f32, b16, dma = jnp.float32, jnp.bfloat16, pltpu.SemaphoreType.DMA
    vmem, hbm = pl.BlockSpec(memory_space=pltpu.VMEM), pl.BlockSpec(memory_space=pl.ANY)
    panel, diagonal = pl.pallas_call(
        functools.partial(kernel, rows_n, cols_n),
        out_shape=(
            jax.ShapeDtypeStruct((rows * chunks, piece), f32),
            jax.ShapeDtypeStruct(pivot_inverse.shape, f32),
        ),
        in_specs=[hbm, hbm, hbm, vmem],
        out_specs=(hbm, vmem),
        scratch_shapes=[
            pltpu.SMEM((supers, structure.shape[0]), jnp.int32),
            pltpu.VMEM((rows * chunks, piece), f32),
            pltpu.VMEM((members, width, width), f32),
            pltpu.VMEM((width, members * width), b16),
            pltpu.VMEM((width, members * width), b16),
            pltpu.VMEM((chunks, rows, piece), f32),
            pltpu.VMEM((supers, 2, width, rows), b16),
            pltpu.VMEM((chunks, rows, piece), f32),
            pltpu.VMEM((chunks, members * cols_n, rows, piece), f32),
            pltpu.VMEM((members * width, 2 * piece), b16),
            pltpu.VMEM((chunks, width, piece), f32),
            pltpu.VMEM((chunks, 2, cols_n - 1, rows, piece), f32),
            pltpu.VMEM((rows * chunks, piece), f32),
            pltpu.VMEM((chunks, PAIR, chips, part, piece), f32),
            pltpu.VMEM((chunks, chips, part, piece), f32),
            pltpu.VMEM((chunks, chips, part, piece), f32),
            pltpu.VMEM((chunks, chips - 1, part, piece), f32),
            pltpu.VMEM((chunks, cuts, part, lanes), f32),
            pltpu.VMEM((chunks, cuts, cols_n, part, lanes), f32),
            dma((4,)),
            dma((8,)),
            dma((2, chunks)),
            dma((chunks,)),
            dma((chunks,)),
            dma((chunks, 2, cols_n - 1)),
            dma((chunks,)),
            dma((chunks,)),
            dma((chunks, cuts)),
        ],
        compiler_params=pltpu.CompilerParams(
            collective_id=0, has_side_effects=True, vmem_limit_bytes=60 * 1024 * 1024
        ),
    )(structure.T, factor, ancestor_inverse, pivot_inverse)
    return panel.reshape(factor_panel.shape), diagonal


def solution(mesh):
    placed = (
        P("prow", "pcol", None, None),
        P("pcol", "prow", None, None),
        P(None, "prow", "pcol"),
        P(),
    )
    return jax.shard_map(
        body,
        mesh=mesh,
        in_specs=placed,
        out_specs=(P("pcol", "prow", None, None), P(None, "prow", "pcol")),
        check_vma=False,
    )
```

```python
import functools

import jax
import jax.numpy as jnp
from jax import lax
from jax.experimental import pallas as pl
from jax.experimental.pallas import tpu as pltpu
from jax.sharding import PartitionSpec as P

MESH = pl.DeviceIdType.MESH
PAIR = 2
PIECE = 128
EAGER = 5
DIRECT = 1
ALONG = (7.0, 1.0)
SPREAD = (11.0, 2.4)
RELAY = 4.0
FORWARD = 3.5
MULTIPLY = 2.0
FIRST_HEAD = -1.0
FINISH = (36.0, 3.9)
HOP = 6.0
LEAD = 4.0
PAIR_TIME = 2.2
CHIPS_TIME = 6.0
CUTS_TIME = 12.0
LATE_CUTS = 4
LATE_TIME = 76.0


def split(value):
    high = value.astype(jnp.bfloat16)
    low = (value - high.astype(jnp.float32)).astype(jnp.bfloat16)
    return high, low


def dot(a, b):
    return lax.dot_general(a, b, (((1,), (0,)), ((), ())), preferred_element_type=jnp.float32)


def flip(value, number, size):
    bit, total = 1, value
    while bit < size:
        if (number // bit) % 2:
            here = lax.rem(lax.div(value, bit), 2)
            total = total + bit - 2 * bit * here
        bit *= 2
    return total


def flip_both(left, right, size):
    bit, total = 1, 0
    while bit < size:
        a, b = lax.rem(lax.div(left, bit), 2), lax.rem(lax.div(right, bit), 2)
        total = total + bit * (a + b - 2 * a * b)
        bit *= 2
    return total


def kernel(
    rows_n,
    cols_n,
    struct_hbm,
    factor_hbm,
    inverse_hbm,
    pivot_ref,
    result_out,
    diag_ref,
    struct,
    raw,
    a_full,
    a_high,
    a_low,
    masked,
    turned,
    staged,
    columns,
    both,
    partial,
    chain_in,
    terms,
    pair_in,
    pair_sum,
    chip_in,
    cut,
    cut_in,
    load_sem,
    sends,
    hop_recv,
    near_recv,
    relay_recv,
    mate_recv,
    chain_recv,
    pair_recv,
    chip_recv,
    cut_recv,
):
    row = lax.axis_index("prow")
    col = lax.axis_index("pcol")
    chunks, rows, piece = masked.shape
    members, width = a_full.shape[0], a_full.shape[1]
    supers = struct.shape[0]
    per_super = width // piece
    chips = rows_n // PAIR
    part = width // rows_n
    lanes = width // cols_n
    cuts = piece // lanes
    core = lax.rem(row, PAIR)
    chip = lax.div(row, PAIR)
    mate = chip * PAIR + (1 - core)
    group = lax.div(row, members)
    member = lax.rem(row, members)
    both_ways = flip_both(group, col, cols_n)

    def other(number):
        return flip(chip, number, chips) * PAIR + core

    besides = (other(1), other(2)) if chips == 4 else None
    across_corner = other(3) if chips == 4 else None

    def direct(k):
        return chips != 4 or k < DIRECT

    load_struct = pltpu.make_async_copy(struct_hbm, struct, load_sem.at[0])
    load_raw = pltpu.make_async_copy(factor_hbm, raw, load_sem.at[1])
    load_a = pltpu.make_async_copy(inverse_hbm.at[0], a_full, load_sem.at[2])
    load_struct.start()
    load_raw.start()
    load_a.start()

    barrier = pltpu.get_barrier_semaphore()
    for step in range(1, rows_n):
        pl.semaphore_signal(
            barrier, inc=1, device_id={"prow": lax.rem(row + step, rows_n)}, device_id_type=MESH
        )
    for step in range(1, cols_n):
        pl.semaphore_signal(
            barrier, inc=1, device_id={"pcol": lax.rem(col + step, cols_n)}, device_id_type=MESH
        )

    def remote(src, dst, send, recv, where):
        return pltpu.make_async_remote_copy(
            src_ref=src, dst_ref=dst, send_sem=send, recv_sem=recv, device_id=where, device_id_type=MESH
        )

    sent = []

    def begin(copy, when=None):
        if when is None:
            copy.start()
        else:
            pl.when(when)(copy.start)
        sent.append((copy, when))

    def across(k):
        to_group = flip(flip_both(group, col, cols_n), k, cols_n)
        stays = flip(col, k, cols_n) == 0
        return (
            remote(
                masked.at[k],
                staged.at[k],
                sends.at[0],
                hop_recv.at[0, k],
                {"prow": to_group * members + member},
            ),
            stays,
        )

    def start_across(k):
        mask = struct[k // per_super, row].astype(jnp.float32)
        value = raw[pl.ds(k, rows, stride=chunks), :] * mask
        masked[k] = value
        copy, stays = across(k)

        @pl.when(stays)
        def _():
            staged[k] = value

        begin(copy, jnp.logical_not(stays))

    def slot_of(source, k):
        from_col = flip(flip_both(lax.div(source, members), col, cols_n), k, cols_n)
        return lax.rem(source, members) * cols_n + from_col

    def along(k):
        to_col = flip(both_ways, k, cols_n)
        copy = remote(
            staged.at[k],
            columns.at[k, member * cols_n + col],
            sends.at[1],
            hop_recv.at[1, k],
            {"pcol": to_col},
        )
        return copy, to_col == col

    def start_along(k):
        copy, stays = across(k)
        pl.when(jnp.logical_not(stays))(copy.wait_recv)
        copy, home = along(k)

        @pl.when(home)
        def _():
            columns[k, member * cols_n + col] = staged[k]

        begin(copy, jnp.logical_not(home))

    def near(k, source, target):
        here = columns.at[k, slot_of(source, k)]
        return remote(here, here, sends.at[2], near_recv.at[k], {"prow": target})

    def over(k, source):
        here = columns.at[k, slot_of(source, k)]
        return remote(here, here, sends.at[3], mate_recv.at[k], {"prow": mate})

    def arrived(buffer, index, count, semaphore):
        here = buffer.at[index, pl.ds(0, count)]
        return remote(here, here, sends.at[0], semaphore, {"prow": mate})

    def back(source, step):
        return lax.rem(source - PAIR * step + rows_n, rows_n)

    def start_spread(k):
        copy, home = along(k)
        pl.when(jnp.logical_not(home))(copy.wait_recv)
        if direct(k):
            for step in range(chips - 1, 0, -1):
                begin(near(k, row, lax.rem(row + PAIR * step, rows_n)))
        else:
            for beside in besides:
                begin(near(k, row, beside))
        begin(over(k, row))

    def relay(k):
        if direct(k):
            return
        arrived(columns, k, 2, near_recv.at[k]).wait_recv()
        half = rows // 2
        for at in (0, 1):
            here = columns.at[k, slot_of(besides[at], k), pl.ds(at * half, half)]
            begin(remote(here, here, sends.at[2], relay_recv.at[k], {"prow": besides[1 - at]}))
            begin(over(k, besides[at]))

    def forward(k):
        if direct(k):
            arrived(columns, k, chips - 1, near_recv.at[k]).wait_recv()
            for step in range(1, chips):
                begin(over(k, back(row, step)))
        else:
            arrived(columns, k, 1, relay_recv.at[k]).wait_recv()
            begin(over(k, across_corner))

    def multiply(k):
        arrived(columns, k, chips, mate_recv.at[k]).wait_recv()
        for index in range(members * cols_n):
            high, low = split(columns[k, index])
            both[index * rows : (index + 1) * rows, :piece] = high
            both[index * rows : (index + 1) * rows, piece:] = low
        first = dot(a_high[...], both[...])
        second = dot(a_low[...], both[:, :piece])
        partial[k] = first[:, :piece] + (first[:, piece:] + second)

    def chain_copy(k, step, side):
        place = col if side == 0 else cols_n - 1 - col
        block = cols_n - 1 - step + place
        block = block if side == 0 else cols_n - 1 - block
        at = pl.ds(pl.multiple_of(block * rows, rows), rows)
        copy = remote(
            partial.at[k, at],
            chain_in.at[k, side, step],
            sends.at[4],
            chain_recv.at[k, side, step],
            {"pcol": col + 1 - 2 * side},
        )
        return copy, at, place

    def came_from(k, step, side):
        return remote(
            chain_in.at[k, side, step],
            chain_in.at[k, side, step],
            sends.at[4],
            chain_recv.at[k, side, step],
            {"pcol": lax.rem(col + 1, cols_n)},
        )

    def chain_start(step, k):
        for side in (0, 1):
            copy, at, place = chain_copy(k, step, side)
            begin(copy, place == 0)

    def chain(step, k):
        for side in (0, 1):
            copy, at, place = chain_copy(k, step, side)
            when = jnp.logical_and(place > 0, place <= step)

            @pl.when(when)
            def _():
                came_from(k, step - 1, side).wait_recv()
                partial[k, at, :] = partial[k, at, :] + chain_in[k, side, step - 1]

            begin(copy, when)

    def finish_panel(k):
        own = pl.ds(pl.multiple_of(col * rows, rows), rows)
        for side in (0, 1):
            place = col if side == 0 else cols_n - 1 - col

            @pl.when(place > 0)
            def _():
                came_from(k, cols_n - 2, side).wait_recv()
                partial[k, own, :] = partial[k, own, :] + chain_in[k, side, cols_n - 2]

        mask = struct[k // per_super, row].astype(jnp.float32)
        result = -mask * partial[k, own, :]
        result_out[pl.ds(k, rows, stride=chunks), :] = result
        high, low = split(result)
        sides = jnp.concatenate([high, low], axis=1)
        first = dot(turned[k // per_super, 0], sides)
        second = dot(turned[k // per_super, 1], high)
        term = first[:, :piece] + (first[:, piece:] + second)
        for at in range(rows_n):
            terms[k, at % PAIR, at // PAIR] = term[at * part : (at + 1) * part]
        begin(pair_copy(k))

    def pair_copy(k):
        return remote(terms.at[k, 1 - core], pair_in.at[k], sends.at[5], pair_recv.at[k], {"prow": mate})

    def chip_copy(k, step):
        to_chip = lax.rem(chip + step, chips)
        return remote(
            pair_sum.at[k, to_chip],
            chip_in.at[k, step - 1],
            sends.at[6],
            chip_recv.at[k],
            {"prow": to_chip * PAIR + core},
        )

    def add_pair(k):
        pair_copy(k).wait_recv()
        pair_sum[k] = terms[k, core] + pair_in[k]
        for step in range(chips - 1, 0, -1):
            begin(chip_copy(k, step))

    def cut_copy(k, at, target):
        step = lax.rem(col - target + cols_n, cols_n)
        return remote(
            cut.at[k, at],
            cut_in.at[k, at, step],
            sends.at[7],
            cut_recv.at[k, at],
            {"pcol": target},
        )

    def add_chips(k):
        total = pair_sum[k, chip]
        arrived(chip_in, k, chips - 1, chip_recv.at[k]).wait_recv()
        for step in range(1, chips):
            total = total + chip_in[k, step - 1]
        for at in range(cuts):
            cut[k, at] = total[:, at * lanes : (at + 1) * lanes]

    def send_cuts(k):
        for at in range(cuts):
            target = k % per_super * cuts + at
            begin(cut_copy(k, at, target), col != target)

    def add_cuts(k):
        for at in range(cuts):

            @pl.when(col == k % per_super * cuts + at)
            def _():
                here = cut_in.at[k, at, pl.ds(1, cols_n - 1)]
                remote(here, here, sends.at[0], cut_recv.at[k, at], {"prow": mate}).wait_recv()
                total = cut[k, at]
                for step in range(1, cols_n):
                    total = total + cut_in[k, at, step]
                diag_ref[k // per_super] = pivot_ref[k // per_super] - total

    def prepare_a():
        load_a.wait()
        for index in range(members):
            high, low = split(a_full[index])
            a_high[:, index * width : (index + 1) * width] = high
            a_low[:, index * width : (index + 1) * width] = low

    def prepare_turned(s):
        for at in range(per_super):
            high, low = split(masked[s * per_super + at].T)
            turned[s, 0, at * piece : (at + 1) * piece] = high
            turned[s, 1, at * piece : (at + 1) * piece] = low

    steps = cols_n - 1
    events = []

    def plan(time, name, stage, k):
        events.append((time, len(events), name, stage, k))

    for k in range(chunks):
        spread_time = SPREAD[0] + SPREAD[1] * k
        forward_time = spread_time + FORWARD + RELAY
        if direct(k):
            forward_time += FIRST_HEAD
        multiply_time = forward_time + MULTIPLY
        finish_time = FINISH[0] + FINISH[1] * k
        chips_time = finish_time + PAIR_TIME + CHIPS_TIME
        if k == chunks - 1:
            chips_time = finish_time + PAIR_TIME
        plan(0.0, "across", start_across, k)
        plan(ALONG[0] + ALONG[1] * k, "along", start_along, k)
        plan(spread_time, "spread", start_spread, k)
        plan(spread_time + RELAY, "relay", relay, k)
        plan(forward_time, "forward", forward, k)
        plan(multiply_time, "multiply", multiply, k)
        for step in range(steps):
            lead = LEAD * step if k >= EAGER else 0.0
            plan(multiply_time + lead, "start", functools.partial(chain_start, step), k)
        for step in range(1, steps):
            chain_time = max(finish_time - HOP * (steps - step), multiply_time + HOP * step)
            plan(chain_time, f"chain{step}", functools.partial(chain, step), k)
        plan(finish_time, "finish", finish_panel, k)
        plan(finish_time + PAIR_TIME, "pair", add_pair, k)
        plan(min(chips_time, FINISH[0] + FINISH[1] * (chunks - 1) + PAIR_TIME), "chips", add_chips, k)
        late = LATE_TIME if k >= LATE_CUTS else 0.0
        plan(max(chips_time, late), "send", send_cuts, k)
        plan(FINISH[0] + FINISH[1] * chunks + 100.0, "cuts", add_cuts, k)
    for s in range(supers):
        plan(SPREAD[0] + 0.2 + s, "turn", prepare_turned, s)
    plan(SPREAD[0] + 0.1, "a", lambda _: prepare_a(), 0)
    events.sort(key=lambda event: event[:2])

    load_struct.wait()
    load_raw.wait()
    pl.semaphore_wait(barrier, rows_n + cols_n - 2)

    for _, _, name, stage, k in events:
        stage(k)

    for copy, when in sent:
        if when is None:
            copy.wait_send()
        else:
            pl.when(when)(copy.wait_send)


def body(ancestor_inverse, factor_panel, pivot_inverse, structure):
    rows_n, cols_n = lax.axis_size("prow"), lax.axis_size("pcol")
    members, width = ancestor_inverse.shape[1], ancestor_inverse.shape[3]
    rows, _, supers, _ = factor_panel.shape
    chips, part, lanes = rows_n // PAIR, width // rows_n, width // cols_n
    piece = max(PIECE, lanes)
    chunks, cuts = supers * width // piece, piece // lanes
    factor = factor_panel.reshape(rows * chunks, piece)
    f32, b16, dma = jnp.float32, jnp.bfloat16, pltpu.SemaphoreType.DMA
    vmem, hbm = pl.BlockSpec(memory_space=pltpu.VMEM), pl.BlockSpec(memory_space=pl.ANY)
    panel, diagonal = pl.pallas_call(
        functools.partial(kernel, rows_n, cols_n),
        out_shape=(
            pltpu.VMEM((rows * chunks, piece), f32),
            pltpu.VMEM(pivot_inverse.shape, f32),
        ),
        in_specs=[hbm, hbm, hbm, vmem],
        out_specs=(vmem, vmem),
        scratch_shapes=[
            pltpu.SMEM((supers, structure.shape[0]), jnp.int32),
            pltpu.VMEM((rows * chunks, piece), f32),
            pltpu.VMEM((members, width, width), f32),
            pltpu.VMEM((width, members * width), b16),
            pltpu.VMEM((width, members * width), b16),
            pltpu.VMEM((chunks, rows, piece), f32),
            pltpu.VMEM((supers, 2, width, rows), b16),
            pltpu.VMEM((chunks, rows, piece), f32),
            pltpu.VMEM((chunks, members * cols_n, rows, piece), f32),
            pltpu.VMEM((members * width, 2 * piece), b16),
            pltpu.VMEM((chunks, width, piece), f32),
            pltpu.VMEM((chunks, 2, cols_n - 1, rows, piece), f32),
            pltpu.VMEM((chunks, PAIR, chips, part, piece), f32),
            pltpu.VMEM((chunks, chips, part, piece), f32),
            pltpu.VMEM((chunks, chips, part, piece), f32),
            pltpu.VMEM((chunks, chips - 1, part, piece), f32),
            pltpu.VMEM((chunks, cuts, part, lanes), f32),
            pltpu.VMEM((chunks, cuts, cols_n, part, lanes), f32),
            dma((3,)),
            dma((8,)),
            dma((2, chunks)),
            dma((chunks,)),
            dma((chunks,)),
            dma((chunks,)),
            dma((chunks, 2, cols_n - 1)),
            dma((chunks,)),
            dma((chunks,)),
            dma((chunks, cuts)),
        ],
        compiler_params=pltpu.CompilerParams(
            collective_id=0, has_side_effects=True, vmem_limit_bytes=62 * 1024 * 1024
        ),
    )(structure.T, factor, ancestor_inverse, pivot_inverse)
    return panel.reshape(factor_panel.shape), diagonal


def solution(mesh):
    placed = (
        P("prow", "pcol", None, None),
        P("pcol", "prow", None, None),
        P(None, "prow", "pcol"),
        P(),
    )
    return jax.shard_map(
        body,
        mesh=mesh,
        in_specs=placed,
        out_specs=(P("pcol", "prow", None, None), P(None, "prow", "pcol")),
        check_vma=False,
    )
```

```python
import functools

import jax
import jax.numpy as jnp
from jax import lax
from jax.experimental import pallas as pl
from jax.experimental.pallas import tpu as pltpu
from jax.sharding import PartitionSpec as P

MESH = pl.DeviceIdType.MESH
PAIR = 2
PIECE = 128
EAGER = 5
DIRECT = 2
BATCH = 12
ACROSS = (4.0, 1.0)
ALONG = (7.0, 0.6)
SPREAD = (11.0, 2.4)
RELAY = 4.0
FORWARD = 3.5
MULTIPLY = 2.0
FIRST_HEAD = -1.0
FINISH = (36.0, 3.9)
HOP = 6.5
LEAD = 4.0
PAIR_TIME = 2.2
CHIPS_TIME = 6.0
CUTS_TIME = 12.0
LATE_CUTS = 4
LATE_TIME = 76.0


def split(value):
    high = value.astype(jnp.bfloat16)
    low = (value - high.astype(jnp.float32)).astype(jnp.bfloat16)
    return high, low


def dot(a, b):
    return lax.dot_general(a, b, (((1,), (0,)), ((), ())), preferred_element_type=jnp.float32)


def flip(value, number, size):
    bit, total = 1, value
    while bit < size:
        if (number // bit) % 2:
            here = lax.rem(lax.div(value, bit), 2)
            total = total + bit - 2 * bit * here
        bit *= 2
    return total


def flip_both(left, right, size):
    bit, total = 1, 0
    while bit < size:
        a, b = lax.rem(lax.div(left, bit), 2), lax.rem(lax.div(right, bit), 2)
        total = total + bit * (a + b - 2 * a * b)
        bit *= 2
    return total


def kernel(
    rows_n,
    cols_n,
    struct_hbm,
    factor_hbm,
    inverse_hbm,
    pivot_ref,
    result_out,
    diag_ref,
    struct,
    raw,
    a_full,
    a_high,
    a_low,
    masked,
    turned,
    staged,
    columns,
    both,
    partial,
    chain_in,
    terms,
    pair_in,
    pair_sum,
    chip_in,
    cut,
    cut_in,
    load_sem,
    sends,
    hop_recv,
    near_recv,
    relay_recv,
    mate_recv,
    chain_recv,
    pair_recv,
    chip_recv,
    cut_recv,
):
    row = lax.axis_index("prow")
    col = lax.axis_index("pcol")
    chunks, rows, piece = masked.shape
    members, width = a_full.shape[0], a_full.shape[1]
    supers = struct.shape[0]
    per_super = width // piece
    chips = rows_n // PAIR
    part = width // rows_n
    lanes = width // cols_n
    cuts = piece // lanes
    core = lax.rem(row, PAIR)
    chip = lax.div(row, PAIR)
    mate = chip * PAIR + (1 - core)
    group = lax.div(row, members)
    member = lax.rem(row, members)
    both_ways = flip_both(group, col, cols_n)

    def other(number):
        return flip(chip, number, chips) * PAIR + core

    besides = (other(1), other(2)) if chips == 4 else None
    across_corner = other(3) if chips == 4 else None

    def direct(k):
        return chips != 4 or k < DIRECT

    load_struct = pltpu.make_async_copy(struct_hbm, struct, load_sem.at[0])
    load_raw = pltpu.make_async_copy(factor_hbm, raw, load_sem.at[1])
    load_a = pltpu.make_async_copy(inverse_hbm.at[0], a_full, load_sem.at[2])
    load_struct.start()
    load_raw.start()
    load_a.start()

    barrier = pltpu.get_barrier_semaphore()
    if members == PAIR:
        greeted = [lax.rem(row + PAIR * step, rows_n) for step in range(1, chips)] + [mate]
    else:
        greeted = [lax.rem(row + step, rows_n) for step in range(1, rows_n)]
    for partner in greeted:
        pl.semaphore_signal(barrier, inc=1, device_id={"prow": partner}, device_id_type=MESH)
    for step in range(1, cols_n):
        pl.semaphore_signal(
            barrier, inc=1, device_id={"pcol": lax.rem(col + step, cols_n)}, device_id_type=MESH
        )

    def remote(src, dst, send, recv, where):
        return pltpu.make_async_remote_copy(
            src_ref=src, dst_ref=dst, send_sem=send, recv_sem=recv, device_id=where, device_id_type=MESH
        )

    sent = []
    even = chunks % cols_n == 0

    def begin(copy, when=None, kept=False):
        if when is None:
            copy.start()
        else:
            pl.when(when)(copy.start)
        if kept:
            sent.append((copy, when))

    def across(k):
        to_group = flip(flip_both(group, col, cols_n), k, cols_n)
        stays = flip(col, k, cols_n) == 0
        return (
            remote(
                masked.at[k],
                staged.at[k],
                sends.at[0],
                hop_recv.at[0, k],
                {"prow": to_group * members + member},
            ),
            stays,
        )

    def start_across(k):
        mask = struct[k // per_super, row].astype(jnp.float32)
        value = raw[pl.ds(k, rows, stride=chunks), :] * mask
        masked[k] = value
        copy, stays = across(k)

        @pl.when(stays)
        def _():
            staged[k] = value

        begin(copy, jnp.logical_not(stays), not even)

    def slot_of(source, k):
        from_col = flip(flip_both(lax.div(source, members), col, cols_n), k, cols_n)
        return lax.rem(source, members) * cols_n + from_col

    def along(k):
        to_col = flip(both_ways, k, cols_n)
        copy = remote(
            staged.at[k],
            columns.at[k, member * cols_n + col],
            sends.at[1],
            hop_recv.at[1, k],
            {"pcol": to_col},
        )
        return copy, to_col == col

    def start_along(k):
        copy, stays = across(k)
        pl.when(jnp.logical_not(stays))(copy.wait_recv)
        copy, home = along(k)

        @pl.when(home)
        def _():
            columns[k, member * cols_n + col] = staged[k]

        begin(copy, jnp.logical_not(home), not even)

    def near(k, source, target):
        here = columns.at[k, slot_of(source, k)]
        return remote(here, here, sends.at[2], near_recv.at[k], {"prow": target})

    def over(k, source):
        here = columns.at[k, slot_of(source, k)]
        return remote(here, here, sends.at[3], mate_recv.at[k], {"prow": mate})

    def arrived(buffer, index, count, semaphore):
        here = buffer.at[index, pl.ds(0, count)]
        return remote(here, here, sends.at[0], semaphore, {"prow": mate})

    def back(source, step):
        return lax.rem(source - PAIR * step + rows_n, rows_n)

    def start_spread(k):
        copy, home = along(k)
        pl.when(jnp.logical_not(home))(copy.wait_recv)
        if direct(k):
            for step in range(chips - 1, 0, -1):
                begin(near(k, row, lax.rem(row + PAIR * step, rows_n)))
        else:
            for beside in besides:
                begin(near(k, row, beside))
        begin(over(k, row))

    def relay(k):
        if direct(k):
            return
        arrived(columns, k, 2, near_recv.at[k]).wait_recv()
        half = rows // 2
        for at in (0, 1):
            here = columns.at[k, slot_of(besides[at], k), pl.ds(at * half, half)]
            begin(remote(here, here, sends.at[2], relay_recv.at[k], {"prow": besides[1 - at]}))
            begin(over(k, besides[at]))

    def forward(k):
        if direct(k):
            arrived(columns, k, chips - 1, near_recv.at[k]).wait_recv()
            for step in range(1, chips):
                begin(over(k, back(row, step)))
        else:
            arrived(columns, k, 1, relay_recv.at[k]).wait_recv()
            begin(over(k, across_corner))

    def multiply(k):
        arrived(columns, k, chips, mate_recv.at[k]).wait_recv()
        for index in range(members * cols_n):
            high, low = split(columns[k, index])
            both[index * rows : (index + 1) * rows, :piece] = high
            both[index * rows : (index + 1) * rows, piece:] = low
        first = dot(a_high[...], both[...])
        second = dot(a_low[...], both[:, :piece])
        partial[k] = first[:, :piece] + (first[:, piece:] + second)

    def chain_copy(k, step, side):
        place = col if side == 0 else cols_n - 1 - col
        block = cols_n - 1 - step + place
        block = block if side == 0 else cols_n - 1 - block
        at = pl.ds(pl.multiple_of(block * rows, rows), rows)
        copy = remote(
            partial.at[k, at],
            chain_in.at[k, side, step],
            sends.at[4],
            chain_recv.at[k, side, step],
            {"pcol": col + 1 - 2 * side},
        )
        return copy, at, place

    def came_from(k, step, side):
        return remote(
            chain_in.at[k, side, step],
            chain_in.at[k, side, step],
            sends.at[4],
            chain_recv.at[k, side, step],
            {"pcol": lax.rem(col + 1, cols_n)},
        )

    def chain_start(step, k):
        for side in (0, 1):
            copy, at, place = chain_copy(k, step, side)
            begin(copy, place == 0)

    def chain(step, k):
        for side in (0, 1):
            copy, at, place = chain_copy(k, step, side)
            when = jnp.logical_and(place > 0, place <= step)

            @pl.when(when)
            def _():
                came_from(k, step - 1, side).wait_recv()
                partial[k, at, :] = partial[k, at, :] + chain_in[k, side, step - 1]

            begin(copy, when)

    def finish_panel(k):
        own = pl.ds(pl.multiple_of(col * rows, rows), rows)
        for side in (0, 1):
            place = col if side == 0 else cols_n - 1 - col

            @pl.when(place > 0)
            def _():
                came_from(k, cols_n - 2, side).wait_recv()
                partial[k, own, :] = partial[k, own, :] + chain_in[k, side, cols_n - 2]

        mask = struct[k // per_super, row].astype(jnp.float32)
        result = -mask * partial[k, own, :]
        result_out[pl.ds(k, rows, stride=chunks), :] = result
        high, low = split(result)
        sides = jnp.concatenate([high, low], axis=1)
        first = dot(turned[k // per_super, 0], sides)
        second = dot(turned[k // per_super, 1], high)
        term = first[:, :piece] + (first[:, piece:] + second)
        for at in range(rows_n):
            terms[k, at % PAIR, at // PAIR] = term[at * part : (at + 1) * part]
        begin(pair_copy(k))

    def pair_copy(k):
        return remote(terms.at[k, 1 - core], pair_in.at[k], sends.at[5], pair_recv.at[k], {"prow": mate})

    def chip_copy(k, step):
        to_chip = lax.rem(chip + step, chips)
        return remote(
            pair_sum.at[k, to_chip],
            chip_in.at[k, step - 1],
            sends.at[6],
            chip_recv.at[k],
            {"prow": to_chip * PAIR + core},
        )

    def add_pair(k):
        pair_copy(k).wait_recv()
        pair_sum[k] = terms[k, core] + pair_in[k]
        for step in range(chips - 1, 0, -1):
            begin(chip_copy(k, step))

    def cut_copy(k, at, target):
        step = lax.rem(col - target + cols_n, cols_n)
        return remote(
            cut.at[k, at],
            cut_in.at[k, at, step],
            sends.at[7],
            cut_recv.at[k, at],
            {"pcol": target},
        )

    def add_chips(k):
        total = pair_sum[k, chip]
        arrived(chip_in, k, chips - 1, chip_recv.at[k]).wait_recv()
        for step in range(1, chips):
            total = total + chip_in[k, step - 1]
        for at in range(cuts):
            cut[k, at] = total[:, at * lanes : (at + 1) * lanes]

    def send_cuts(k):
        for at in range(cuts):
            target = k % per_super * cuts + at
            begin(cut_copy(k, at, target), col != target)

    def add_cuts(k):
        for at in range(cuts):

            @pl.when(col == k % per_super * cuts + at)
            def _():
                here = cut_in.at[k, at, pl.ds(1, cols_n - 1)]
                remote(here, here, sends.at[0], cut_recv.at[k, at], {"prow": mate}).wait_recv()
                total = cut[k, at]
                for step in range(1, cols_n):
                    total = total + cut_in[k, at, step]
                diag_ref[k // per_super] = pivot_ref[k // per_super] - total

    def prepare_a():
        load_a.wait()
        for index in range(members):
            high, low = split(a_full[index])
            a_high[:, index * width : (index + 1) * width] = high
            a_low[:, index * width : (index + 1) * width] = low

    def prepare_turned(s):
        for at in range(per_super):
            high, low = split(masked[s * per_super + at].T)
            turned[s, 0, at * piece : (at + 1) * piece] = high
            turned[s, 1, at * piece : (at + 1) * piece] = low

    steps = cols_n - 1
    events = []

    def plan(time, name, stage, k):
        events.append((time, len(events), name, stage, k))

    for k in range(chunks):
        spread_time = SPREAD[0] + SPREAD[1] * k
        forward_time = spread_time + FORWARD + RELAY
        if direct(k):
            forward_time += FIRST_HEAD
        multiply_time = forward_time + MULTIPLY
        finish_time = FINISH[0] + FINISH[1] * k
        chips_time = finish_time + PAIR_TIME + CHIPS_TIME
        if k == chunks - 1:
            chips_time = finish_time + PAIR_TIME
        plan(ACROSS[0] + ACROSS[1] * k if k >= BATCH else 0.0, "across", start_across, k)
        plan(ALONG[0] + ALONG[1] * k, "along", start_along, k)
        plan(spread_time, "spread", start_spread, k)
        plan(spread_time + RELAY, "relay", relay, k)
        plan(forward_time, "forward", forward, k)
        plan(multiply_time, "multiply", multiply, k)
        for step in range(steps):
            lead = LEAD * step if k >= EAGER else 0.0
            plan(multiply_time + lead, "start", functools.partial(chain_start, step), k)
        for step in range(1, steps):
            chain_time = max(finish_time - HOP * (steps - step), multiply_time + HOP * step)
            plan(chain_time, f"chain{step}", functools.partial(chain, step), k)
        plan(finish_time, "finish", finish_panel, k)
        plan(finish_time + PAIR_TIME, "pair", add_pair, k)
        plan(min(chips_time, FINISH[0] + FINISH[1] * (chunks - 1) + PAIR_TIME + 0.1), "chips", add_chips, k)
        late = LATE_TIME if k >= LATE_CUTS else 0.0
        plan(max(chips_time, late), "send", send_cuts, k)
        plan(FINISH[0] + FINISH[1] * chunks + 100.0, "cuts", add_cuts, k)
    for s in range(supers):
        plan(FINISH[0] - 3.0 + s, "turn", prepare_turned, s)
    plan(SPREAD[0] + 0.1, "a", lambda _: prepare_a(), 0)
    events.sort(key=lambda event: event[:2])

    load_struct.wait()
    load_raw.wait()
    pl.semaphore_wait(barrier, len(greeted) + cols_n - 1)

    for _, _, name, stage, k in events:
        stage(k)

    moved = pl.ds(0, chunks - chunks // cols_n)
    totals = [
        (2, columns.at[:, pl.ds(0, chips - 1)]),
        (3, columns.at[:, pl.ds(0, chips)]),
        (4, chain_in.at[:, 0]),
        (5, pair_in),
        (6, chip_in),
        (7, cut_in.at[pl.ds(0, supers), 0, pl.ds(0, cols_n - 1)]),
    ]
    if even:
        totals += [(0, masked.at[moved]), (1, masked.at[moved])]
    for kind, total in totals:
        remote(total, total, sends.at[kind], near_recv.at[0], {"prow": mate}).wait_send()
    for copy, when in sent:
        pl.when(when)(copy.wait_send)


def body(ancestor_inverse, factor_panel, pivot_inverse, structure):
    rows_n, cols_n = lax.axis_size("prow"), lax.axis_size("pcol")
    members, width = ancestor_inverse.shape[1], ancestor_inverse.shape[3]
    rows, _, supers, _ = factor_panel.shape
    chips, part, lanes = rows_n // PAIR, width // rows_n, width // cols_n
    piece = max(PIECE, lanes)
    chunks, cuts = supers * width // piece, piece // lanes
    factor = factor_panel.reshape(rows * chunks, piece)
    f32, b16, dma = jnp.float32, jnp.bfloat16, pltpu.SemaphoreType.DMA
    vmem, hbm = pl.BlockSpec(memory_space=pltpu.VMEM), pl.BlockSpec(memory_space=pl.ANY)
    panel, diagonal = pl.pallas_call(
        functools.partial(kernel, rows_n, cols_n),
        out_shape=(
            pltpu.VMEM((rows * chunks, piece), f32),
            pltpu.VMEM(pivot_inverse.shape, f32),
        ),
        in_specs=[hbm, hbm, hbm, vmem],
        out_specs=(vmem, vmem),
        scratch_shapes=[
            pltpu.SMEM((supers, structure.shape[0]), jnp.int32),
            pltpu.VMEM((rows * chunks, piece), f32),
            pltpu.VMEM((members, width, width), f32),
            pltpu.VMEM((width, members * width), b16),
            pltpu.VMEM((width, members * width), b16),
            pltpu.VMEM((chunks, rows, piece), f32),
            pltpu.VMEM((supers, 2, width, rows), b16),
            pltpu.VMEM((chunks, rows, piece), f32),
            pltpu.VMEM((chunks, members * cols_n, rows, piece), f32),
            pltpu.VMEM((members * width, 2 * piece), b16),
            pltpu.VMEM((chunks, width, piece), f32),
            pltpu.VMEM((chunks, 2, cols_n - 1, rows, piece), f32),
            pltpu.VMEM((chunks, PAIR, chips, part, piece), f32),
            pltpu.VMEM((chunks, chips, part, piece), f32),
            pltpu.VMEM((chunks, chips, part, piece), f32),
            pltpu.VMEM((chunks, chips - 1, part, piece), f32),
            pltpu.VMEM((chunks, cuts, part, lanes), f32),
            pltpu.VMEM((chunks, cuts, cols_n, part, lanes), f32),
            dma((3,)),
            dma((8,)),
            dma((2, chunks)),
            dma((chunks,)),
            dma((chunks,)),
            dma((chunks,)),
            dma((chunks, 2, cols_n - 1)),
            dma((chunks,)),
            dma((chunks,)),
            dma((chunks, cuts)),
        ],
        compiler_params=pltpu.CompilerParams(
            collective_id=0, has_side_effects=True, vmem_limit_bytes=62 * 1024 * 1024
        ),
    )(structure.T, factor, ancestor_inverse, pivot_inverse)
    return panel.reshape(factor_panel.shape), diagonal


def solution(mesh):
    placed = (
        P("prow", "pcol", None, None),
        P("pcol", "prow", None, None),
        P(None, "prow", "pcol"),
        P(),
    )
    return jax.shard_map(
        body,
        mesh=mesh,
        in_specs=placed,
        out_specs=(P("pcol", "prow", None, None), P(None, "prow", "pcol")),
        check_vma=False,
    )
```

```python
import functools

import jax
import jax.numpy as jnp
from jax import lax
from jax.experimental import pallas as pl
from jax.experimental.pallas import tpu as pltpu
from jax.sharding import PartitionSpec as P

MESH = pl.DeviceIdType.MESH
PAIR = 2
PIECE = 128
EAGER = 5
DIRECT = 2
BATCH = 12
ACROSS = (4.0, 1.0)
ALONG = (7.0, 0.6)
SPREAD = (11.0, 2.4)
RELAY = 4.0
FORWARD = 3.5
MULTIPLY = 2.0
FIRST_HEAD = -1.0
FINISH = (36.0, 3.9)
HOP = 7.0
LEAD = 4.0
PAIR_TIME = 2.2
CHIPS_TIME = 6.0
CUTS_TIME = 12.0
LATE_CUTS = 4
LATE_TIME = 76.0


def split(value):
    high = value.astype(jnp.bfloat16)
    low = (value - high.astype(jnp.float32)).astype(jnp.bfloat16)
    return high, low


def dot(a, b):
    return lax.dot_general(a, b, (((1,), (0,)), ((), ())), preferred_element_type=jnp.float32)


def flip(value, number, size):
    bit, total = 1, value
    while bit < size:
        if (number // bit) % 2:
            here = lax.rem(lax.div(value, bit), 2)
            total = total + bit - 2 * bit * here
        bit *= 2
    return total


def flip_both(left, right, size):
    bit, total = 1, 0
    while bit < size:
        a, b = lax.rem(lax.div(left, bit), 2), lax.rem(lax.div(right, bit), 2)
        total = total + bit * (a + b - 2 * a * b)
        bit *= 2
    return total


def kernel(
    rows_n,
    cols_n,
    struct_hbm,
    factor_hbm,
    inverse_hbm,
    pivot_ref,
    result_out,
    diag_ref,
    struct,
    raw,
    a_full,
    a_high,
    a_low,
    masked,
    turned,
    staged,
    columns,
    both,
    partial,
    chain_in,
    terms,
    pair_in,
    pair_sum,
    chip_in,
    cut,
    cut_in,
    load_sem,
    sends,
    hop_recv,
    near_recv,
    relay_recv,
    mate_recv,
    chain_recv,
    pair_recv,
    chip_recv,
    cut_recv,
):
    row = lax.axis_index("prow")
    col = lax.axis_index("pcol")
    chunks, rows, piece = masked.shape
    members, width = a_full.shape[0], a_full.shape[1]
    supers = struct.shape[0]
    per_super = width // piece
    chips = rows_n // PAIR
    part = width // rows_n
    lanes = width // cols_n
    cuts = piece // lanes
    core = lax.rem(row, PAIR)
    chip = lax.div(row, PAIR)
    mate = chip * PAIR + (1 - core)
    group = lax.div(row, members)
    member = lax.rem(row, members)
    both_ways = flip_both(group, col, cols_n)

    def other(number):
        return flip(chip, number, chips) * PAIR + core

    besides = (other(1), other(2)) if chips == 4 else None
    across_corner = other(3) if chips == 4 else None

    def direct(k):
        return chips != 4 or k < DIRECT

    load_struct = pltpu.make_async_copy(struct_hbm, struct, load_sem.at[0])
    load_raw = pltpu.make_async_copy(factor_hbm, raw, load_sem.at[1])
    load_a = pltpu.make_async_copy(inverse_hbm.at[0], a_full, load_sem.at[2])
    load_struct.start()
    load_raw.start()
    load_a.start()

    barrier = pltpu.get_barrier_semaphore()
    if members == PAIR:
        greeted = [lax.rem(row + PAIR * step, rows_n) for step in range(1, chips)] + [mate]
    else:
        greeted = [lax.rem(row + step, rows_n) for step in range(1, rows_n)]
    for partner in greeted:
        pl.semaphore_signal(barrier, inc=1, device_id={"prow": partner}, device_id_type=MESH)
    for step in range(1, cols_n):
        pl.semaphore_signal(
            barrier, inc=1, device_id={"pcol": lax.rem(col + step, cols_n)}, device_id_type=MESH
        )

    def remote(src, dst, send, recv, where):
        return pltpu.make_async_remote_copy(
            src_ref=src, dst_ref=dst, send_sem=send, recv_sem=recv, device_id=where, device_id_type=MESH
        )

    sent = []
    even = chunks % cols_n == 0

    def begin(copy, when=None, kept=False):
        if when is None:
            copy.start()
        else:
            pl.when(when)(copy.start)
        if kept:
            sent.append((copy, when))

    def across(k):
        to_group = flip(flip_both(group, col, cols_n), k, cols_n)
        stays = flip(col, k, cols_n) == 0
        return (
            remote(
                masked.at[k],
                staged.at[k],
                sends.at[0],
                hop_recv.at[0, k],
                {"prow": to_group * members + member},
            ),
            stays,
        )

    def start_across(k):
        mask = struct[k // per_super, row].astype(jnp.float32)
        value = raw[pl.ds(k, rows, stride=chunks), :] * mask
        masked[k] = value
        copy, stays = across(k)

        @pl.when(stays)
        def _():
            staged[k] = value

        begin(copy, jnp.logical_not(stays), not even)

    def slot_of(source, k):
        from_col = flip(flip_both(lax.div(source, members), col, cols_n), k, cols_n)
        return lax.rem(source, members) * cols_n + from_col

    def along(k):
        to_col = flip(both_ways, k, cols_n)
        copy = remote(
            staged.at[k],
            columns.at[k, member * cols_n + col],
            sends.at[1],
            hop_recv.at[1, k],
            {"pcol": to_col},
        )
        return copy, to_col == col

    def start_along(k):
        copy, stays = across(k)
        pl.when(jnp.logical_not(stays))(copy.wait_recv)
        copy, home = along(k)

        @pl.when(home)
        def _():
            columns[k, member * cols_n + col] = staged[k]

        begin(copy, jnp.logical_not(home), not even)

    def near(k, source, target):
        here = columns.at[k, slot_of(source, k)]
        return remote(here, here, sends.at[2], near_recv.at[k], {"prow": target})

    def over(k, source):
        here = columns.at[k, slot_of(source, k)]
        return remote(here, here, sends.at[3], mate_recv.at[k], {"prow": mate})

    def arrived(buffer, index, count, semaphore):
        here = buffer.at[index, pl.ds(0, count)]
        return remote(here, here, sends.at[0], semaphore, {"prow": mate})

    def back(source, step):
        return lax.rem(source - PAIR * step + rows_n, rows_n)

    def start_spread(k):
        copy, home = along(k)
        pl.when(jnp.logical_not(home))(copy.wait_recv)
        if direct(k):
            for step in range(chips - 1, 0, -1):
                begin(near(k, row, lax.rem(row + PAIR * step, rows_n)))
        else:
            for beside in besides:
                begin(near(k, row, beside))
        begin(over(k, row))

    def relay(k):
        if direct(k):
            return
        arrived(columns, k, 2, near_recv.at[k]).wait_recv()
        half = rows // 2
        for at in (0, 1):
            here = columns.at[k, slot_of(besides[at], k), pl.ds(at * half, half)]
            begin(remote(here, here, sends.at[2], relay_recv.at[k], {"prow": besides[1 - at]}))
            begin(over(k, besides[at]))

    def forward(k):
        if direct(k):
            arrived(columns, k, chips - 1, near_recv.at[k]).wait_recv()
            for step in range(1, chips):
                begin(over(k, back(row, step)))
        else:
            arrived(columns, k, 1, relay_recv.at[k]).wait_recv()
            begin(over(k, across_corner))

    def multiply(k):
        arrived(columns, k, chips, mate_recv.at[k]).wait_recv()
        for index in range(members * cols_n):
            high, low = split(columns[k, index])
            both[index * rows : (index + 1) * rows, :piece] = high
            both[index * rows : (index + 1) * rows, piece:] = low
        first = dot(a_high[...], both[...])
        second = dot(a_low[...], both[:, :piece])
        partial[k] = first[:, :piece] + (first[:, piece:] + second)

    def chain_copy(k, step, side):
        place = col if side == 0 else cols_n - 1 - col
        block = cols_n - 1 - step + place
        block = block if side == 0 else cols_n - 1 - block
        at = pl.ds(pl.multiple_of(block * rows, rows), rows)
        copy = remote(
            partial.at[k, at],
            chain_in.at[k, side, step],
            sends.at[4],
            chain_recv.at[k, side, step],
            {"pcol": col + 1 - 2 * side},
        )
        return copy, at, place

    def came_from(k, step, side):
        return remote(
            chain_in.at[k, side, step],
            chain_in.at[k, side, step],
            sends.at[4],
            chain_recv.at[k, side, step],
            {"pcol": lax.rem(col + 1, cols_n)},
        )

    def chain_start(step, k):
        for side in (0, 1):
            copy, at, place = chain_copy(k, step, side)
            begin(copy, place == 0)

    def chain(step, k):
        for side in (0, 1):
            copy, at, place = chain_copy(k, step, side)
            when = jnp.logical_and(place > 0, place <= step)

            @pl.when(when)
            def _():
                came_from(k, step - 1, side).wait_recv()
                partial[k, at, :] = partial[k, at, :] + chain_in[k, side, step - 1]

            begin(copy, when)

    def finish_panel(k):
        own = pl.ds(pl.multiple_of(col * rows, rows), rows)
        for side in (0, 1):
            place = col if side == 0 else cols_n - 1 - col

            @pl.when(place > 0)
            def _():
                came_from(k, cols_n - 2, side).wait_recv()
                partial[k, own, :] = partial[k, own, :] + chain_in[k, side, cols_n - 2]

        mask = struct[k // per_super, row].astype(jnp.float32)
        result = -mask * partial[k, own, :]
        result_out[pl.ds(k, rows, stride=chunks), :] = result
        high, low = split(result)
        sides = jnp.concatenate([high, low], axis=1)
        first = dot(turned[k // per_super, 0], sides)
        second = dot(turned[k // per_super, 1], high)
        term = first[:, :piece] + (first[:, piece:] + second)
        for at in range(rows_n):
            terms[k, at % PAIR, at // PAIR] = term[at * part : (at + 1) * part]
        begin(pair_copy(k))

    def pair_copy(k):
        return remote(terms.at[k, 1 - core], pair_in.at[k], sends.at[5], pair_recv.at[k], {"prow": mate})

    def chip_copy(k, step):
        to_chip = lax.rem(chip + step, chips)
        return remote(
            pair_sum.at[k, to_chip],
            chip_in.at[k, step - 1],
            sends.at[6],
            chip_recv.at[k],
            {"prow": to_chip * PAIR + core},
        )

    def add_pair(k):
        pair_copy(k).wait_recv()
        pair_sum[k] = terms[k, core] + pair_in[k]
        for step in range(chips - 1, 0, -1):
            begin(chip_copy(k, step))

    def cut_copy(k, at, target):
        step = lax.rem(col - target + cols_n, cols_n)
        return remote(
            cut.at[k, at],
            cut_in.at[k, at, step],
            sends.at[7],
            cut_recv.at[k, at],
            {"pcol": target},
        )

    def add_chips(k):
        total = pair_sum[k, chip]
        arrived(chip_in, k, chips - 1, chip_recv.at[k]).wait_recv()
        for step in range(1, chips):
            total = total + chip_in[k, step - 1]
        for at in range(cuts):
            cut[k, at] = total[:, at * lanes : (at + 1) * lanes]

    def send_cuts(k):
        for at in range(cuts):
            target = k % per_super * cuts + at
            begin(cut_copy(k, at, target), col != target)

    def add_cuts(k):
        for at in range(cuts):

            @pl.when(col == k % per_super * cuts + at)
            def _():
                here = cut_in.at[k, at, pl.ds(1, cols_n - 1)]
                remote(here, here, sends.at[0], cut_recv.at[k, at], {"prow": mate}).wait_recv()
                total = cut[k, at]
                for step in range(1, cols_n):
                    total = total + cut_in[k, at, step]
                diag_ref[k // per_super] = pivot_ref[k // per_super] - total

    def prepare_a():
        load_a.wait()
        for index in range(members):
            high, low = split(a_full[index])
            a_high[:, index * width : (index + 1) * width] = high
            a_low[:, index * width : (index + 1) * width] = low

    def prepare_turned(s):
        for at in range(per_super):
            high, low = split(masked[s * per_super + at].T)
            turned[s, 0, at * piece : (at + 1) * piece] = high
            turned[s, 1, at * piece : (at + 1) * piece] = low

    steps = cols_n - 1
    events = []

    def plan(time, name, stage, k):
        events.append((time, len(events), name, stage, k))

    for k in range(chunks):
        spread_time = SPREAD[0] + SPREAD[1] * k
        forward_time = spread_time + FORWARD + RELAY
        if direct(k):
            forward_time += FIRST_HEAD
        multiply_time = forward_time + MULTIPLY
        finish_time = FINISH[0] + FINISH[1] * k
        chips_time = finish_time + PAIR_TIME + CHIPS_TIME
        if k == chunks - 1:
            chips_time = finish_time + PAIR_TIME
        plan(ACROSS[0] + ACROSS[1] * k if k >= BATCH else 0.0, "across", start_across, k)
        plan(ALONG[0] + ALONG[1] * k, "along", start_along, k)
        plan(spread_time, "spread", start_spread, k)
        plan(spread_time + RELAY, "relay", relay, k)
        plan(forward_time, "forward", forward, k)
        plan(multiply_time, "multiply", multiply, k)
        for step in range(steps):
            lead = LEAD * step if k >= EAGER else 0.0
            plan(multiply_time + lead, "start", functools.partial(chain_start, step), k)
        for step in range(1, steps):
            chain_time = max(finish_time - HOP * (steps - step), multiply_time + HOP * step)
            plan(chain_time, f"chain{step}", functools.partial(chain, step), k)
        plan(finish_time, "finish", finish_panel, k)
        plan(finish_time + PAIR_TIME, "pair", add_pair, k)
        plan(min(chips_time, FINISH[0] + FINISH[1] * (chunks - 1) + PAIR_TIME + 0.1), "chips", add_chips, k)
        late = LATE_TIME if k >= LATE_CUTS else 0.0
        plan(max(chips_time, late), "send", send_cuts, k)
        plan(FINISH[0] + FINISH[1] * chunks + 100.0, "cuts", add_cuts, k)
    for s in range(supers):
        plan(FINISH[0] - 3.0 + s, "turn", prepare_turned, s)
    plan(SPREAD[0] + 0.1, "a", lambda _: prepare_a(), 0)
    events.sort(key=lambda event: event[:2])

    load_struct.wait()
    load_raw.wait()
    pl.semaphore_wait(barrier, len(greeted) + cols_n - 1)

    for _, _, name, stage, k in events:
        stage(k)

    moved = pl.ds(0, chunks - chunks // cols_n)
    totals = [
        (2, columns.at[:, pl.ds(0, chips - 1)]),
        (3, columns.at[:, pl.ds(0, chips)]),
        (4, chain_in.at[:, 0]),
        (5, pair_in),
        (6, chip_in),
        (7, cut_in.at[pl.ds(0, supers), 0, pl.ds(0, cols_n - 1)]),
    ]
    if even:
        totals += [(0, masked.at[moved]), (1, masked.at[moved])]
    for kind, total in totals:
        remote(total, total, sends.at[kind], near_recv.at[0], {"prow": mate}).wait_send()
    for copy, when in sent:
        pl.when(when)(copy.wait_send)


def body(ancestor_inverse, factor_panel, pivot_inverse, structure):
    rows_n, cols_n = lax.axis_size("prow"), lax.axis_size("pcol")
    members, width = ancestor_inverse.shape[1], ancestor_inverse.shape[3]
    rows, _, supers, _ = factor_panel.shape
    chips, part, lanes = rows_n // PAIR, width // rows_n, width // cols_n
    piece = max(PIECE, lanes)
    chunks, cuts = supers * width // piece, piece // lanes
    factor = factor_panel.reshape(rows * chunks, piece)
    f32, b16, dma = jnp.float32, jnp.bfloat16, pltpu.SemaphoreType.DMA
    vmem, hbm = pl.BlockSpec(memory_space=pltpu.VMEM), pl.BlockSpec(memory_space=pl.ANY)
    panel, diagonal = pl.pallas_call(
        functools.partial(kernel, rows_n, cols_n),
        out_shape=(
            pltpu.VMEM((rows * chunks, piece), f32),
            pltpu.VMEM(pivot_inverse.shape, f32),
        ),
        in_specs=[hbm, hbm, hbm, vmem],
        out_specs=(vmem, vmem),
        scratch_shapes=[
            pltpu.SMEM((supers, structure.shape[0]), jnp.int32),
            pltpu.VMEM((rows * chunks, piece), f32),
            pltpu.VMEM((members, width, width), f32),
            pltpu.VMEM((width, members * width), b16),
            pltpu.VMEM((width, members * width), b16),
            pltpu.VMEM((chunks, rows, piece), f32),
            pltpu.VMEM((supers, 2, width, rows), b16),
            pltpu.VMEM((chunks, rows, piece), f32),
            pltpu.VMEM((chunks, members * cols_n, rows, piece), f32),
            pltpu.VMEM((members * width, 2 * piece), b16),
            pltpu.VMEM((chunks, width, piece), f32),
            pltpu.VMEM((chunks, 2, cols_n - 1, rows, piece), f32),
            pltpu.VMEM((chunks, PAIR, chips, part, piece), f32),
            pltpu.VMEM((chunks, chips, part, piece), f32),
            pltpu.VMEM((chunks, chips, part, piece), f32),
            pltpu.VMEM((chunks, chips - 1, part, piece), f32),
            pltpu.VMEM((chunks, cuts, part, lanes), f32),
            pltpu.VMEM((chunks, cuts, cols_n, part, lanes), f32),
            dma((3,)),
            dma((8,)),
            dma((2, chunks)),
            dma((chunks,)),
            dma((chunks,)),
            dma((chunks,)),
            dma((chunks, 2, cols_n - 1)),
            dma((chunks,)),
            dma((chunks,)),
            dma((chunks, cuts)),
        ],
        compiler_params=pltpu.CompilerParams(
            collective_id=0, has_side_effects=True, vmem_limit_bytes=62 * 1024 * 1024
        ),
    )(structure.T, factor, ancestor_inverse, pivot_inverse)
    return panel.reshape(factor_panel.shape), diagonal


def solution(mesh):
    placed = (
        P("prow", "pcol", None, None),
        P("pcol", "prow", None, None),
        P(None, "prow", "pcol"),
        P(),
    )
    return jax.shard_map(
        body,
        mesh=mesh,
        in_specs=placed,
        out_specs=(P("pcol", "prow", None, None), P(None, "prow", "pcol")),
        check_vma=False,
    )
```
